32 devices in a mesh: task: 2 (over x), dp: 8 (over z, core), mp: 2 (over y).
Axes of the slice: x: 2, y: 2, z: 4, core: 2. Of those that a mesh axis runs over, the one named last changes fastest.
Arguments:
- deltas: bfloat16 [6, 2048, 4608], P('task', 'dp', 'mp'), may hold values from -400 to 400, as said below
- fishers: bfloat16 [6, 2048, 4608], P('task', 'dp', 'mp'), may hold values from 0.0009994507 to 1
Outputs:
- merged_out: float32 [2048, 4608], P('dp', 'mp')
The draws below stay inside these ranges and needn't reach their ends.
Inputs may be any that keep to these rules, and one draw needn't show every extreme that they name: `deltas`: Real-valued weight differences.
All inputs are finite; a program needn't handle non-finite values.
Results may differ from the reference program's by a relative error of at most 0.0003.
Values sent between devices are 32-bit elements; how exact they have to be, the bound alone decides.
A program may use at most 64 MiB of HBM per device.

```python
import math
import jax
import jax.numpy as jnp
from jax import lax

D = 4608
ROW_DEV = 256
ROWS = 2048
TASKS = 6


def draw_deltas(key, part):
    keys = jax.random.split(jax.random.fold_in(key, 11), 5)
    row_index = jnp.arange(ROWS, dtype=jnp.int32)
    row_pos = row_index.astype(jnp.float32) / ROWS
    inner_pos = (row_index % ROW_DEV).astype(jnp.float32) / ROW_DEV
    col_pos = jnp.arange(D, dtype=jnp.float32) / D
    noise = jnp.clip(jax.random.normal(keys[0], (TASKS, ROWS, D), jnp.float32), -6.0, 6.0)
    row_rise = 3.0 ** (row_pos - 0.5) * 3.0 ** (inner_pos - 0.5)
    row_scale = jnp.exp(jax.random.uniform(keys[2], (ROWS,), jnp.float32, 0.0, math.log(10.0))) / 4.6 * row_rise
    col_scale = jnp.exp(jax.random.uniform(keys[3], (D,), jnp.float32, 0.0, math.log(10.0))) / 4.6 * 3.0 ** (col_pos - 0.5)
    task_scale = jnp.exp(jax.random.uniform(keys[4], (TASKS,), jnp.float32, -0.7, 0.7))
    values = noise * row_scale[None, :, None] * col_scale[None, None, :] * task_scale[:, None, None]
    return values.astype(jnp.bfloat16)


def shard_levels(own_key, shape, pieces, least, top_value):
    level, own = 1.0, jax.random.fold_in(own_key, 6)
    for dim, parts in pieces:
        draws = jnp.exp(jax.random.uniform(jax.random.fold_in(own, dim), (parts,), jnp.float32, least / len(pieces), top_value / len(pieces)))
        level = level * jnp.repeat(draws, shape[dim] // parts).reshape([-1 if axis == dim else 1 for axis in range(len(shape))])
    return level


def setup_inputs(seed: int = 0) -> dict:
    seeds = jax.random.split(jax.random.key(seed), 3)
    return {
        "deltas": draw_deltas(jax.random.fold_in(seeds[2], 71), 0),
        "fishers": jnp.clip(jnp.exp(math.log(1.0) - 6.9083047 * jax.random.uniform(seeds[1], (TASKS, ROWS, D), jnp.float32) ** shard_levels(seeds[1], (TASKS, ROWS, D), ((0, 2), (1, 8), (2, 2)), -0.2, 0.2)), 0.0009994507, 1.0).astype(jnp.bfloat16),
    }


def reference(deltas, fishers):
    weights = fishers.astype(jnp.float32)
    widened = deltas.astype(jnp.float32)
    numerator = lax.optimization_barrier(jnp.sum(weights * widened, axis=0))
    denominator = lax.optimization_barrier(jnp.sum(weights, axis=0))
    merged = numerator / denominator
    task_sq = lax.optimization_barrier(jnp.sum(widened * widened, axis=(1, 2)))
    merged_sq = jnp.sum(merged * merged)
    rescale = jnp.mean(jnp.sqrt(task_sq + 1e-06)) / jnp.sqrt(merged_sq + 1e-06)
    return rescale * merged
```

```python
import functools

import jax
import jax.numpy as jnp
from jax import lax
from jax.experimental import pallas as pl
from jax.experimental.pallas import tpu as pltpu
from jax.sharding import PartitionSpec as P

MESH = pl.DeviceIdType.MESH
ROW_STEP = 16
COL_STEP = 256
EARLY_REPLIES = 2


def exchange_steps(mesh):
    steps = []
    for axis in ("task", "mp", "dp"):
        size = mesh.shape[axis]
        assert size & (size - 1) == 0
        bit = 1
        while bit < size:
            steps.append((axis, bit))
            bit *= 2
    return steps


def peer_of(axis, bit):
    me = lax.axis_index(axis)
    return me + bit - 2 * bit * (me // bit % 2)


def kernel(steps, tasks, deltas, fishers, out, delta_v, fisher_v, sent, own, landed, merged, reply,
           staged, squares, merged_squares, sums, sums_in, load_sem, send_sem, recv_sem, reply_send, reply_recv,
           sum_send, sum_recv, store_sem):
    held, rows, cols = delta_v.shape
    half = rows // 2
    pieces = half // ROW_STEP
    me = lax.axis_index("task")
    partner = {"task": peer_of("task", 1)}
    mine_base = me * half
    other_base = (1 - me) * half
    blocks = [(at, min(COL_STEP, cols - at)) for at in range(0, cols, COL_STEP)]

    def row_at(base, c):
        return pl.ds(pl.multiple_of(base + c * ROW_STEP, ROW_STEP), ROW_STEP)

    def load(side, c):
        at = row_at(other_base if side == 0 else mine_base, c)
        return (
            pltpu.make_async_copy(deltas.at[:, at, :], delta_v.at[:, at, :], load_sem.at[side, 0, c]),
            pltpu.make_async_copy(fishers.at[:, at, :], fisher_v.at[:, at, :], load_sem.at[side, 1, c]),
        )

    def send(c):
        return pltpu.make_async_remote_copy(
            src_ref=sent.at[c], dst_ref=landed.at[c], send_sem=send_sem.at[c], recv_sem=recv_sem.at[c],
            device_id=partner, device_id_type=MESH)

    def answer(c):
        return pltpu.make_async_remote_copy(
            src_ref=merged.at[c], dst_ref=reply.at[c], send_sem=reply_send.at[c], recv_sem=reply_recv.at[c],
            device_id=partner, device_id_type=MESH)

    def exchange(s):
        axis, bit = steps[s]
        return pltpu.make_async_remote_copy(
            src_ref=sums.at[s], dst_ref=sums_in.at[s], send_sem=sum_send.at[s], recv_sem=sum_recv.at[s],
            device_id={axis: peer_of(axis, bit)}, device_id_type=MESH)

    def store(base, c):
        at = row_at(base, c)
        return pltpu.make_async_copy(staged.at[at, :], out.at[at, :], store_sem.at[base // half, c])

    for side in range(2):
        @pl.loop(0, pieces)
        def _(c):
            for copy in load(side, c):
                copy.start()

    barrier = pltpu.get_barrier_semaphore()
    for axis, bit in steps:
        pl.semaphore_signal(barrier, inc=1, device_id={axis: peer_of(axis, bit)}, device_id_type=MESH)

    squares[...] = jnp.zeros_like(squares)
    merged_squares[...] = jnp.zeros_like(merged_squares)

    def partial(side, c, target):
        for copy in load(side, c):
            copy.wait()
        at = row_at(other_base if side == 0 else mine_base, c)
        for start, width in blocks:
            span = pl.ds(start, width)
            numerator = denominator = None
            for k in range(held):
                weight = fisher_v[k, at, span].astype(jnp.float32)
                value = delta_v[k, at, span].astype(jnp.float32)
                squares[k, :, span] += value * value
                numerator = weight * value if k == 0 else numerator + weight * value
                denominator = weight if k == 0 else denominator + weight
            target[c, 0, :, span] = numerator
            target[c, 1, :, span] = denominator

    partial(0, 0, sent)
    pl.semaphore_wait(barrier, len(steps))

    @pl.loop(1, pieces)
    def _(c):
        partial(0, c, sent)
        send(c - 1).start()

    partial(1, 0, own)
    send(pieces - 1).start()

    @pl.loop(1, pieces)
    def _(c):
        partial(1, c, own)

    def merge(c):
        send(c).wait_recv()
        for start, width in blocks:
            span = pl.ds(start, width)
            value = (own[c, 0, :, span] + landed[c, 0, :, span]) / (own[c, 1, :, span] + landed[c, 1, :, span])
            merged[c, :, span] = value
            merged_squares[:, span] += value * value

    merge(0)

    @pl.loop(1, pieces)
    def _(c):
        merge(c)

        @pl.when(c <= EARLY_REPLIES)
        def _():
            answer(c - 1).start()

    index = lax.broadcasted_iota(jnp.int32, sums.shape[1:], 0)
    totals = jnp.where(index == tasks, jnp.sum(merged_squares[...]), 0.0)
    for k in range(held):
        totals = jnp.where(index == me * held + k, jnp.sum(squares[k]), totals)
    for s in range(len(steps)):
        sums[s] = totals
        exchange(s).start()
        if s == 0:
            @pl.loop(EARLY_REPLIES, pieces)
            def _(c):
                answer(c).start()
        exchange(s).wait_recv()
        totals = totals + sums_in[s]

    roots = jnp.sqrt(totals + 1e-06)
    target = jnp.sum(jnp.where(index < tasks, roots, 0.0), axis=0, keepdims=True) / tasks
    norm = jnp.sum(jnp.where(index == tasks, roots, 0.0), axis=0, keepdims=True)
    rescale = jnp.max(target / norm)

    @pl.loop(0, pieces)
    def _(c):
        at = row_at(mine_base, c)
        for start, width in blocks:
            span = pl.ds(start, width)
            staged[at, span] = merged[c, :, span] * rescale
        store(mine_base, c).start()

    @pl.loop(0, pieces)
    def _(c):
        answer(c).wait_recv()
        at = row_at(other_base, c)
        for start, width in blocks:
            span = pl.ds(start, width)
            staged[at, span] = reply[c, :, span] * rescale
        store(other_base, c).start()

    for s in range(len(steps)):
        exchange(s).wait_send()

    @pl.loop(0, pieces)
    def _(c):
        send(c).wait_send()
        answer(c).wait_send()
        store(mine_base, c).wait()
        store(other_base, c).wait()


def shards(mesh, deltas, fishers):
    held, rows, cols = deltas.shape
    assert mesh.shape["task"] == 2 and rows % (2 * ROW_STEP) == 0
    steps = exchange_steps(mesh)
    tasks = held * mesh.shape["task"]
    pieces = rows // 2 // ROW_STEP
    sum_rows = (tasks + 8) // 8 * 8
    f32 = jnp.float32
    dma = pltpu.SemaphoreType.DMA
    return pl.pallas_call(
        functools.partial(kernel, steps, tasks),
        out_shape=jax.ShapeDtypeStruct((rows, cols), f32),
        in_specs=[pl.BlockSpec(memory_space=pl.ANY)] * 2,
        out_specs=pl.BlockSpec(memory_space=pl.ANY),
        scratch_shapes=[
            pltpu.VMEM(deltas.shape, deltas.dtype),
            pltpu.VMEM(fishers.shape, fishers.dtype),
            pltpu.VMEM((pieces, 2, ROW_STEP, cols), f32),
            pltpu.VMEM((pieces, 2, ROW_STEP, cols), f32),
            pltpu.VMEM((pieces, 2, ROW_STEP, cols), f32),
            pltpu.VMEM((pieces, ROW_STEP, cols), f32),
            pltpu.VMEM((pieces, ROW_STEP, cols), f32),
            pltpu.VMEM((rows, cols), f32),
            pltpu.VMEM((held, ROW_STEP, cols), f32),
            pltpu.VMEM((ROW_STEP, cols), f32),
            pltpu.VMEM((len(steps), sum_rows, 128), f32),
            pltpu.VMEM((len(steps), sum_rows, 128), f32),
            dma((2, 2, pieces)),
            dma((pieces,)),
            dma((pieces,)),
            dma((pieces,)),
            dma((pieces,)),
            dma((len(steps),)),
            dma((len(steps),)),
            dma((2, pieces)),
        ],
        compiler_params=pltpu.CompilerParams(collective_id=0, has_side_effects=True),
        name="merge",
    )(deltas, fishers)


def solution(mesh):
    placed = (P("task", "dp", "mp"), P("task", "dp", "mp"))
    return jax.shard_map(
        functools.partial(shards, mesh), mesh=mesh, in_specs=placed, out_specs=P("dp", "mp"), check_vma=False
    )
```

```python
import functools

import jax
import jax.numpy as jnp
from jax import lax
from jax.experimental import pallas as pl
from jax.experimental.pallas import tpu as pltpu
from jax.sharding import PartitionSpec as P

MESH = pl.DeviceIdType.MESH
ROW_STEP = 16
COL_STEP = 256
EARLY_REPLIES = 2


def exchange_steps(mesh):
    steps = []
    for axis in ("task", "mp", "dp"):
        size = mesh.shape[axis]
        assert size & (size - 1) == 0
        bit = 1
        while bit < size:
            steps.append((axis, bit))
            bit *= 2
    return steps


def peer_of(axis, bit):
    me = lax.axis_index(axis)
    return me + bit - 2 * bit * (me // bit % 2)


def kernel(steps, tasks, deltas, fishers, out, delta_v, fisher_v, sent, own, landed, merged, reply,
           squares, merged_squares, sums, sums_in, load_sem, send_sem, recv_sem, reply_send, reply_recv,
           sum_send, sum_recv):
    held, rows, cols = delta_v.shape
    half = rows // 2
    pieces = half // ROW_STEP
    me = lax.axis_index("task")
    partner = {"task": peer_of("task", 1)}
    mine_base = me * half
    other_base = (1 - me) * half
    blocks = [(at, min(COL_STEP, cols - at)) for at in range(0, cols, COL_STEP)]

    def row_at(base, c):
        return pl.ds(pl.multiple_of(base + c * ROW_STEP, ROW_STEP), ROW_STEP)

    def load(side, c):
        at = row_at(other_base if side == 0 else mine_base, c)
        return (
            pltpu.make_async_copy(deltas.at[:, at, :], delta_v.at[:, at, :], load_sem.at[side, 0, c]),
            pltpu.make_async_copy(fishers.at[:, at, :], fisher_v.at[:, at, :], load_sem.at[side, 1, c]),
        )

    def send(c):
        return pltpu.make_async_remote_copy(
            src_ref=sent.at[c], dst_ref=landed.at[c], send_sem=send_sem.at[c], recv_sem=recv_sem.at[c],
            device_id=partner, device_id_type=MESH)

    def answer(c):
        return pltpu.make_async_remote_copy(
            src_ref=merged.at[c], dst_ref=reply.at[c], send_sem=reply_send.at[c], recv_sem=reply_recv.at[c],
            device_id=partner, device_id_type=MESH)

    def exchange(s):
        axis, bit = steps[s]
        return pltpu.make_async_remote_copy(
            src_ref=sums.at[s], dst_ref=sums_in.at[s], send_sem=sum_send.at[s], recv_sem=sum_recv.at[s],
            device_id={axis: peer_of(axis, bit)}, device_id_type=MESH)

    for copy in load(0, 0):
        copy.start()

    barrier = pltpu.get_barrier_semaphore()
    for axis, bit in steps:
        pl.semaphore_signal(barrier, inc=1, device_id={axis: peer_of(axis, bit)}, device_id_type=MESH)

    for side in range(2):
        @pl.loop(1 - side, pieces)
        def _(c):
            for copy in load(side, c):
                copy.start()

    squares[...] = jnp.zeros_like(squares)
    merged_squares[...] = jnp.zeros_like(merged_squares)

    def partial(side, c, target):
        for copy in load(side, c):
            copy.wait()
        at = row_at(other_base if side == 0 else mine_base, c)
        for start, width in blocks:
            span = pl.ds(start, width)
            numerator = denominator = None
            for k in range(held):
                weight = fisher_v[k, at, span].astype(jnp.float32)
                value = delta_v[k, at, span].astype(jnp.float32)
                squares[k, :, span] += value * value
                numerator = weight * value if k == 0 else numerator + weight * value
                denominator = weight if k == 0 else denominator + weight
            target[c, 0, :, span] = numerator
            target[c, 1, :, span] = denominator

    partial(0, 0, sent)
    pl.semaphore_wait(barrier, len(steps))
    send(0).start()
    partial(0, 1, sent)

    @pl.loop(2, pieces)
    def _(c):
        partial(0, c, sent)
        send(c - 1).start()

    partial(1, 0, own)
    send(pieces - 1).start()

    @pl.loop(1, pieces)
    def _(c):
        partial(1, c, own)

    def merge(c):
        send(c).wait_recv()
        for start, width in blocks:
            span = pl.ds(start, width)
            value = (own[c, 0, :, span] + landed[c, 0, :, span]) / (own[c, 1, :, span] + landed[c, 1, :, span])
            merged[c, :, span] = value
            merged_squares[:, span] += value * value

    merge(0)

    @pl.loop(1, pieces)
    def _(c):
        merge(c)

        @pl.when(c <= EARLY_REPLIES)
        def _():
            answer(c - 1).start()

    index = lax.broadcasted_iota(jnp.int32, sums.shape[1:], 0)
    totals = jnp.where(index == tasks, jnp.sum(merged_squares[...]), 0.0)
    for k in range(held):
        totals = jnp.where(index == me * held + k, jnp.sum(squares[k]), totals)
    for s in range(len(steps)):
        sums[s] = totals
        exchange(s).start()
        if s == 0:
            @pl.loop(EARLY_REPLIES, pieces)
            def _(c):
                answer(c).start()
        exchange(s).wait_recv()
        totals = totals + sums_in[s]

    roots = jnp.sqrt(totals + 1e-06)
    target = jnp.sum(jnp.where(index < tasks, roots, 0.0), axis=0, keepdims=True) / tasks
    norm = jnp.sum(jnp.where(index == tasks, roots, 0.0), axis=0, keepdims=True)
    rescale = jnp.max(target / norm)

    @pl.loop(0, pieces)
    def _(c):
        at = row_at(mine_base, c)
        for start, width in blocks:
            span = pl.ds(start, width)
            out[at, span] = merged[c, :, span] * rescale

    @pl.loop(0, pieces)
    def _(c):
        answer(c).wait_recv()
        at = row_at(other_base, c)
        for start, width in blocks:
            span = pl.ds(start, width)
            out[at, span] = reply[c, :, span] * rescale

    for s in range(len(steps)):
        exchange(s).wait_send()

    @pl.loop(0, pieces)
    def _(c):
        send(c).wait_send()
        answer(c).wait_send()


def shards(mesh, deltas, fishers):
    held, rows, cols = deltas.shape
    assert mesh.shape["task"] == 2 and rows % (2 * ROW_STEP) == 0
    steps = exchange_steps(mesh)
    tasks = held * mesh.shape["task"]
    pieces = rows // 2 // ROW_STEP
    sum_rows = (tasks + 8) // 8 * 8
    f32 = jnp.float32
    dma = pltpu.SemaphoreType.DMA
    return pl.pallas_call(
        functools.partial(kernel, steps, tasks),
        out_shape=pltpu.VMEM((rows, cols), f32),
        in_specs=[pl.BlockSpec(memory_space=pltpu.HBM)] * 2,
        out_specs=pl.BlockSpec(memory_space=pltpu.VMEM),
        scratch_shapes=[
            pltpu.VMEM(deltas.shape, deltas.dtype),
            pltpu.VMEM(fishers.shape, fishers.dtype),
            pltpu.VMEM((pieces, 2, ROW_STEP, cols), f32),
            pltpu.VMEM((pieces, 2, ROW_STEP, cols), f32),
            pltpu.VMEM((pieces, 2, ROW_STEP, cols), f32),
            pltpu.VMEM((pieces, ROW_STEP, cols), f32),
            pltpu.VMEM((pieces, ROW_STEP, cols), f32),
            pltpu.VMEM((held, ROW_STEP, cols), f32),
            pltpu.VMEM((ROW_STEP, cols), f32),
            pltpu.VMEM((len(steps), sum_rows, 128), f32),
            pltpu.VMEM((len(steps), sum_rows, 128), f32),
            dma((2, 2, pieces)),
            dma((pieces,)),
            dma((pieces,)),
            dma((pieces,)),
            dma((pieces,)),
            dma((len(steps),)),
            dma((len(steps),)),
        ],
        compiler_params=pltpu.CompilerParams(collective_id=0, has_side_effects=True, vmem_limit_bytes=32 * 1024 * 1024),
        name="merge",
    )(*(pltpu.with_memory_space_constraint(x, pltpu.HBM) for x in (deltas, fishers)))


def solution(mesh):
    placed = (P("task", "dp", "mp"), P("task", "dp", "mp"))
    return jax.shard_map(
        functools.partial(shards, mesh), mesh=mesh, in_specs=placed, out_specs=P("dp", "mp"), check_vma=False
    )
```

```python
import functools

import jax
import jax.numpy as jnp
from jax import lax
from jax.experimental import pallas as pl
from jax.experimental.pallas import tpu as pltpu
from jax.sharding import PartitionSpec as P

MESH = pl.DeviceIdType.MESH
ROW_STEP = 16
COL_STEP = 256
CORES = 2
EARLY_REPLIES = 2


def exchange_steps(mesh):
    steps = []
    for axis, size in (("task", mesh.shape["task"]), ("mp", mesh.shape["mp"]), ("dp", CORES)):
        assert size & (size - 1) == 0
        bit = 1
        while bit < size:
            steps.append((axis, bit))
            bit *= 2
    return steps


def peer_of(axis, bit):
    me = lax.axis_index(axis)
    return me + bit - 2 * bit * (me // bit % 2)


def kernel(steps, chips, tasks, deltas, fishers, out, delta_v, fisher_v, sent, own, landed, merged, reply,
           squares, merged_squares, sums, sums_in, load_sem, send_sem, recv_sem, reply_send, reply_recv,
           sum_send, sum_recv,
           line, line_in, line_send, line_recv, head_load, head_send, head_recv):
    held, rows, cols = delta_v.shape
    half = rows // 2
    pieces = half // ROW_STEP
    me = lax.axis_index("task")
    partner = {"task": peer_of("task", 1)}
    mine_base = me * half
    other_base = (1 - me) * half
    blocks = [(at, min(COL_STEP, cols - at)) for at in range(0, cols, COL_STEP)]

    def row_at(base, c):
        return pl.ds(pl.multiple_of(base + c * ROW_STEP, ROW_STEP), ROW_STEP)

    def load(side, c):
        at = row_at(other_base if side == 0 else mine_base, c)
        return (
            pltpu.make_async_copy(deltas.at[:, at, :], delta_v.at[:, at, :], load_sem.at[side, 0, c]),
            pltpu.make_async_copy(fishers.at[:, at, :], fisher_v.at[:, at, :], load_sem.at[side, 1, c]),
        )

    def send(c):
        return pltpu.make_async_remote_copy(
            src_ref=sent.at[c], dst_ref=landed.at[c], send_sem=send_sem.at[c], recv_sem=recv_sem.at[c],
            device_id=partner, device_id_type=MESH)

    def answer(c):
        return pltpu.make_async_remote_copy(
            src_ref=merged.at[c], dst_ref=reply.at[c], send_sem=reply_send.at[c], recv_sem=reply_recv.at[c],
            device_id=partner, device_id_type=MESH)

    first = 2 * COL_STEP if cols > 2 * COL_STEP and cols % 128 == 0 else cols
    parts = [(0, first)] + ([(first, cols - first)] if first < cols else [])

    def head_loads(p):
        at = row_at(other_base, 0)
        span = pl.ds(*parts[p])
        return (
            pltpu.make_async_copy(deltas.at[:, at, span], delta_v.at[:, at, span], head_load.at[0, p]),
            pltpu.make_async_copy(fishers.at[:, at, span], fisher_v.at[:, at, span], head_load.at[1, p]),
        )

    def send_head(p):
        span = pl.ds(*parts[p])
        return pltpu.make_async_remote_copy(
            src_ref=sent.at[0, :, :, span], dst_ref=landed.at[0, :, :, span], send_sem=head_send.at[p],
            recv_sem=head_recv.at[p], device_id=partner, device_id_type=MESH)

    row = lax.axis_index("dp")
    chip = row // CORES
    has_next = (jnp.bool_(True), chip < chips - 1, chip > 0)

    def pass_on(way):
        to = lax.rem(row + way * CORES + chips * CORES, chips * CORES)
        slot = 0 if way == 1 else 1
        return pltpu.make_async_remote_copy(
            src_ref=line.at[slot], dst_ref=line_in.at[slot], send_sem=line_send.at[slot],
            recv_sem=line_recv.at[slot], device_id={"dp": to}, device_id_type=MESH)

    def exchange(s):
        axis, bit = steps[s]
        return pltpu.make_async_remote_copy(
            src_ref=sums.at[s], dst_ref=sums_in.at[s], send_sem=sum_send.at[s], recv_sem=sum_recv.at[s],
            device_id={axis: peer_of(axis, bit)}, device_id_type=MESH)

    line_in[...] = jnp.zeros_like(line_in)
    for p in range(len(parts)):
        for copy in head_loads(p):
            copy.start()

    barrier = pltpu.get_barrier_semaphore()
    for axis, bit in steps:
        pl.semaphore_signal(barrier, inc=1, device_id={axis: peer_of(axis, bit)}, device_id_type=MESH)
    for way in (1, -1):
        @pl.when(has_next[way])
        def _():
            pl.semaphore_signal(
                barrier, inc=1, device_id={"dp": row + way * CORES}, device_id_type=MESH)

    for side in range(2):
        @pl.loop(1 - side, pieces)
        def _(c):
            for copy in load(side, c):
                copy.start()

    squares[...] = jnp.zeros_like(squares)
    merged_squares[...] = jnp.zeros_like(merged_squares)

    def partial(side, c, target):
        for copy in load(side, c):
            copy.wait()
        combine(side, c, target, blocks)

    def combine(side, c, target, chosen):
        at = row_at(other_base if side == 0 else mine_base, c)
        for start, width in chosen:
            span = pl.ds(start, width)
            numerator = denominator = None
            for k in range(held):
                weight = fisher_v[k, at, span].astype(jnp.float32)
                value = delta_v[k, at, span].astype(jnp.float32)
                squares[k, :, span] += value * value
                numerator = weight * value if k == 0 else numerator + weight * value
                denominator = weight if k == 0 else denominator + weight
            target[c, 0, :, span] = numerator
            target[c, 1, :, span] = denominator

    for p, (low, size) in enumerate(parts):
        for copy in head_loads(p):
            copy.wait()
        combine(0, 0, sent, [block for block in blocks if low <= block[0] < low + size])
        if p == 0:
            pl.semaphore_wait(barrier, len(steps) + has_next[1].astype(jnp.int32) + has_next[-1].astype(jnp.int32))
            send_head(0).start()
    partial(0, 1, sent)
    for p in range(1, len(parts)):
        send_head(p).start()

    @pl.loop(2, pieces)
    def _(c):
        partial(0, c, sent)
        send(c - 1).start()

    partial(1, 0, own)
    send(pieces - 1).start()

    @pl.loop(1, pieces)
    def _(c):
        partial(1, c, own)

    def merge(c):
        for start, width in blocks:
            span = pl.ds(start, width)
            value = (own[c, 0, :, span] + landed[c, 0, :, span]) / (own[c, 1, :, span] + landed[c, 1, :, span])
            merged[c, :, span] = value
            merged_squares[:, span] += value * value

    for p in range(len(parts)):
        send_head(p).wait_recv()
    merge(0)

    @pl.loop(1, pieces)
    def _(c):
        send(c).wait_recv()
        merge(c)

        @pl.when(c <= EARLY_REPLIES)
        def _():
            answer(c - 1).start()

    index = lax.broadcasted_iota(jnp.int32, sums.shape[1:], 0)
    totals = jnp.where(index == tasks, jnp.sum(merged_squares[...]), 0.0)
    for k in range(held):
        totals = jnp.where(index == me * held + k, jnp.sum(squares[k]), totals)
    for s in range(len(steps)):
        sums[s] = totals
        exchange(s).start()
        if s == 0:
            @pl.loop(EARLY_REPLIES, pieces)
            def _(c):
                answer(c).start()
        exchange(s).wait_recv()
        totals = totals + sums_in[s]

    def sweep(way):
        slot = 0 if way == 1 else 1

        @pl.when(has_next[-way])
        def _():
            pass_on(way).wait_recv()

        @pl.when(has_next[way])
        def _():
            line[slot] = line_in[slot] + totals
            pass_on(way).start()

    @pl.when(chip < chips // 2)
    def _():
        sweep(1)
        sweep(-1)

    @pl.when(chip >= chips // 2)
    def _():
        sweep(-1)
        sweep(1)

    totals = totals + line_in[0] + line_in[1]
    roots = jnp.sqrt(totals + 1e-06)
    target = jnp.sum(jnp.where(index < tasks, roots, 0.0), axis=0, keepdims=True) / tasks
    norm = jnp.sum(jnp.where(index == tasks, roots, 0.0), axis=0, keepdims=True)
    rescale = jnp.max(target / norm)

    @pl.loop(0, pieces)
    def _(c):
        at = row_at(mine_base, c)
        for start, width in blocks:
            span = pl.ds(start, width)
            out[at, span] = merged[c, :, span] * rescale

    @pl.loop(0, pieces)
    def _(c):
        answer(c).wait_recv()
        at = row_at(other_base, c)
        for start, width in blocks:
            span = pl.ds(start, width)
            out[at, span] = reply[c, :, span] * rescale

    for s in range(len(steps)):
        exchange(s).wait_send()

    for way in (1, -1):
        @pl.when(has_next[way])
        def _():
            pass_on(way).wait_send()

    for p in range(len(parts)):
        send_head(p).wait_send()

    @pl.loop(0, pieces)
    def _(c):
        answer(c).wait_send()

        @pl.when(c > 0)
        def _():
            send(c).wait_send()


def shards(mesh, deltas, fishers):
    held, rows, cols = deltas.shape
    assert mesh.shape["task"] == 2 and rows % (2 * ROW_STEP) == 0
    steps = exchange_steps(mesh)
    tasks = held * mesh.shape["task"]
    pieces = rows // 2 // ROW_STEP
    sum_rows = (tasks + 8) // 8 * 8
    f32 = jnp.float32
    dma = pltpu.SemaphoreType.DMA
    return pl.pallas_call(
        functools.partial(kernel, steps, mesh.shape["dp"] // CORES, tasks),
        out_shape=pltpu.VMEM((rows, cols), f32),
        in_specs=[pl.BlockSpec(memory_space=pltpu.HBM)] * 2,
        out_specs=pl.BlockSpec(memory_space=pltpu.VMEM),
        scratch_shapes=[
            pltpu.VMEM(deltas.shape, deltas.dtype),
            pltpu.VMEM(fishers.shape, fishers.dtype),
            pltpu.VMEM((pieces, 2, ROW_STEP, cols), f32),
            pltpu.VMEM((pieces, 2, ROW_STEP, cols), f32),
            pltpu.VMEM((pieces, 2, ROW_STEP, cols), f32),
            pltpu.VMEM((pieces, ROW_STEP, cols), f32),
            pltpu.VMEM((pieces, ROW_STEP, cols), f32),
            pltpu.VMEM((held, ROW_STEP, cols), f32),
            pltpu.VMEM((ROW_STEP, cols), f32),
            pltpu.VMEM((len(steps), sum_rows, 128), f32),
            pltpu.VMEM((len(steps), sum_rows, 128), f32),
            dma((2, 2, pieces)),
            dma((pieces,)),
            dma((pieces,)),
            dma((pieces,)),
            dma((pieces,)),
            dma((len(steps),)),
            dma((len(steps),)),
            pltpu.VMEM((2, sum_rows, 128), f32),
            pltpu.VMEM((2, sum_rows, 128), f32),
            dma((2,)),
            dma((2,)),
            dma((2, 2)),
            dma((2,)),
            dma((2,)),
        ],
        compiler_params=pltpu.CompilerParams(collective_id=0, has_side_effects=True, vmem_limit_bytes=32 * 1024 * 1024),
        name="merge",
    )(*(pltpu.with_memory_space_constraint(x, pltpu.HBM) for x in (deltas, fishers)))


def solution(mesh):
    placed = (P("task", "dp", "mp"), P("task", "dp", "mp"))
    return jax.shard_map(
        functools.partial(shards, mesh), mesh=mesh, in_specs=placed, out_specs=P("dp", "mp"), check_vma=False
    )
```

```python
import functools

import jax
import jax.numpy as jnp
from jax import lax
from jax.experimental import pallas as pl
from jax.experimental.pallas import tpu as pltpu
from jax.sharding import PartitionSpec as P

MESH = pl.DeviceIdType.MESH
ROW_STEP = 16
COL_STEP = 256
CORES = 2
EARLY_REPLIES = 2


def exchange_steps(mesh):
    steps = []
    for axis, size in (("task", mesh.shape["task"]), ("mp", mesh.shape["mp"]), ("dp", CORES)):
        assert size & (size - 1) == 0
        bit = 1
        while bit < size:
            steps.append((axis, bit))
            bit *= 2
    return steps


def peer_of(axis, bit):
    me = lax.axis_index(axis)
    return me + bit - 2 * bit * (me // bit % 2)


def strip_cut(cols):
    return cols * 2 // 3 // COL_STEP * COL_STEP if cols >= 3 * COL_STEP and cols % 128 == 0 else cols


def kernel(steps, chips, tasks, deltas, fishers, out, delta_v, fisher_v, sent, own, landed, merged, reply,
           squares, merged_squares, sums, sums_in, load_sem, send_sem, recv_sem, reply_send, reply_recv,
           sum_send, sum_recv,
           line, line_in, line_send, line_recv, head_load, head_send, head_recv,
           strip_in=None, strip_merged=None, strip_reply=None, strip_send=None, strip_recv=None):
    held, rows, cols = delta_v.shape
    half = rows // 2
    pieces = half // ROW_STEP
    me = lax.axis_index("task")
    partner = {"task": peer_of("task", 1)}
    mine_base = me * half
    other_base = (1 - me) * half
    blocks = [(at, min(COL_STEP, cols - at)) for at in range(0, cols, COL_STEP)]

    def row_at(base, c):
        return pl.ds(pl.multiple_of(base + c * ROW_STEP, ROW_STEP), ROW_STEP)

    def load(side, c):
        at = row_at(other_base if side == 0 else mine_base, c)
        return (
            pltpu.make_async_copy(deltas.at[:, at, :], delta_v.at[:, at, :], load_sem.at[side, 0, c]),
            pltpu.make_async_copy(fishers.at[:, at, :], fisher_v.at[:, at, :], load_sem.at[side, 1, c]),
        )

    def send(c):
        return pltpu.make_async_remote_copy(
            src_ref=sent.at[c], dst_ref=landed.at[c], send_sem=send_sem.at[c], recv_sem=recv_sem.at[c],
            device_id=partner, device_id_type=MESH)

    def answer(c):
        return pltpu.make_async_remote_copy(
            src_ref=merged.at[c], dst_ref=reply.at[c], send_sem=reply_send.at[c], recv_sem=reply_recv.at[c],
            device_id=partner, device_id_type=MESH)

    first = 2 * COL_STEP if cols > 2 * COL_STEP and cols % 128 == 0 else cols
    parts = [(0, first)] + ([(first, cols - first)] if first < cols else [])

    def head_loads(p):
        at = row_at(other_base, 0)
        span = pl.ds(*parts[p])
        return (
            pltpu.make_async_copy(deltas.at[:, at, span], delta_v.at[:, at, span], head_load.at[0, p]),
            pltpu.make_async_copy(fishers.at[:, at, span], fisher_v.at[:, at, span], head_load.at[1, p]),
        )

    def send_head(p):
        span = pl.ds(*parts[p])
        return pltpu.make_async_remote_copy(
            src_ref=sent.at[0, :, :, span], dst_ref=landed.at[0, :, :, span], send_sem=head_send.at[p],
            recv_sem=head_recv.at[p], device_id=partner, device_id_type=MESH)

    last = pieces - 1
    cut = strip_cut(cols)
    strip = cols - cut
    low, high = pl.ds(0, cut), pl.ds(cut, strip)
    low_blocks = [block for block in blocks if block[0] < cut]
    leading = me == 0

    def roles(of_leading, of_other):
        pl.when(leading)(of_leading)
        pl.when(jnp.logical_not(leading))(of_other)

    def send_low():
        return pltpu.make_async_remote_copy(
            src_ref=sent.at[last, :, :, low], dst_ref=landed.at[last, :, :, low], send_sem=send_sem.at[last],
            recv_sem=recv_sem.at[last], device_id=partner, device_id_type=MESH)

    def answer_low():
        return pltpu.make_async_remote_copy(
            src_ref=merged.at[last, :, low], dst_ref=reply.at[last, :, low], send_sem=reply_send.at[last],
            recv_sem=reply_recv.at[last], device_id=partner, device_id_type=MESH)

    def send_strip():
        return pltpu.make_async_remote_copy(
            src_ref=own.at[last, :, :, high], dst_ref=strip_in, send_sem=strip_send.at[0],
            recv_sem=strip_recv.at[0], device_id=partner, device_id_type=MESH)

    def answer_strip():
        return pltpu.make_async_remote_copy(
            src_ref=strip_merged, dst_ref=strip_reply, send_sem=strip_send.at[1],
            recv_sem=strip_recv.at[1], device_id=partner, device_id_type=MESH)

    row = lax.axis_index("dp")
    chip = row // CORES
    has_next = (jnp.bool_(True), chip < chips - 1, chip > 0)

    def pass_on(way):
        to = lax.rem(row + way * CORES + chips * CORES, chips * CORES)
        slot = 0 if way == 1 else 1
        return pltpu.make_async_remote_copy(
            src_ref=line.at[slot], dst_ref=line_in.at[slot], send_sem=line_send.at[slot],
            recv_sem=line_recv.at[slot], device_id={"dp": to}, device_id_type=MESH)

    def exchange(s):
        axis, bit = steps[s]
        return pltpu.make_async_remote_copy(
            src_ref=sums.at[s], dst_ref=sums_in.at[s], send_sem=sum_send.at[s], recv_sem=sum_recv.at[s],
            device_id={axis: peer_of(axis, bit)}, device_id_type=MESH)

    line_in[...] = jnp.zeros_like(line_in)
    for p in range(len(parts)):
        for copy in head_loads(p):
            copy.start()

    barrier = pltpu.get_barrier_semaphore()
    for axis, bit in steps:
        pl.semaphore_signal(barrier, inc=1, device_id={axis: peer_of(axis, bit)}, device_id_type=MESH)
    for way in (1, -1):
        @pl.when(has_next[way])
        def _():
            pl.semaphore_signal(
                barrier, inc=1, device_id={"dp": row + way * CORES}, device_id_type=MESH)

    for side in range(2):
        @pl.loop(1 - side, pieces)
        def _(c):
            for copy in load(side, c):
                copy.start()

    squares[...] = jnp.zeros_like(squares)
    merged_squares[...] = jnp.zeros_like(merged_squares)

    def partial(side, c, target):
        for copy in load(side, c):
            copy.wait()
        combine(side, c, target, blocks)

    def combine(side, c, target, chosen):
        at = row_at(other_base if side == 0 else mine_base, c)
        for start, width in chosen:
            span = pl.ds(start, width)
            numerator = denominator = None
            for k in range(held):
                weight = fisher_v[k, at, span].astype(jnp.float32)
                value = delta_v[k, at, span].astype(jnp.float32)
                squares[k, :, span] += value * value
                numerator = weight * value if k == 0 else numerator + weight * value
                denominator = weight if k == 0 else denominator + weight
            target[c, 0, :, span] = numerator
            target[c, 1, :, span] = denominator

    for p, (begin, size) in enumerate(parts):
        for copy in head_loads(p):
            copy.wait()
        combine(0, 0, sent, [block for block in blocks if begin <= block[0] < begin + size])
        if p == 0:
            pl.semaphore_wait(barrier, len(steps) + has_next[1].astype(jnp.int32) + has_next[-1].astype(jnp.int32))
            send_head(0).start()
    partial(0, 1, sent)
    for p in range(1, len(parts)):
        send_head(p).start()

    @pl.loop(2, pieces)
    def _(c):
        partial(0, c, sent)
        send(c - 1).start()

    partial(1, 0, own)
    roles(lambda: send(last).start(), lambda: send_low().start())

    @pl.loop(1, pieces)
    def _(c):
        partial(1, c, own)

    if strip:
        @pl.when(leading)
        def _():
            send_strip().start()

    def merge(c, chosen=blocks):
        for start, width in chosen:
            span = pl.ds(start, width)
            value = (own[c, 0, :, span] + landed[c, 0, :, span]) / (own[c, 1, :, span] + landed[c, 1, :, span])
            merged[c, :, span] = value
            merged_squares[:, span] += value * value

    for p in range(len(parts)):
        send_head(p).wait_recv()
    merge(0)

    @pl.loop(1, last)
    def _(c):
        send(c).wait_recv()
        merge(c)

        @pl.when(c <= EARLY_REPLIES)
        def _():
            answer(c - 1).start()

    def merge_low():
        send_low().wait_recv()
        merge(last, low_blocks)

    def merge_last():
        send(last).wait_recv()
        merge(last)
        if strip:
            send_strip().wait_recv()
            value = (sent[last, 0, :, high] + strip_in[0]) / (sent[last, 1, :, high] + strip_in[1])
            strip_merged[...] = value
            merged_squares[:, high] += value * value

    roles(merge_low, merge_last)

    index = lax.broadcasted_iota(jnp.int32, sums.shape[1:], 0)
    totals = jnp.where(index == tasks, jnp.sum(merged_squares[...]), 0.0)
    for k in range(held):
        totals = jnp.where(index == me * held + k, jnp.sum(squares[k]), totals)
    for s in range(len(steps)):
        sums[s] = totals
        exchange(s).start()
        if s == 0:
            @pl.loop(EARLY_REPLIES, last)
            def _(c):
                answer(c).start()

            def answer_last():
                answer(last).start()
                if strip:
                    answer_strip().start()

            roles(lambda: answer_low().start(), answer_last)
        exchange(s).wait_recv()
        totals = totals + sums_in[s]

    def sweep(way):
        slot = 0 if way == 1 else 1

        @pl.when(has_next[-way])
        def _():
            pass_on(way).wait_recv()

        @pl.when(has_next[way])
        def _():
            line[slot] = line_in[slot] + totals
            pass_on(way).start()

    @pl.when(chip < chips // 2)
    def _():
        sweep(1)
        sweep(-1)

    @pl.when(chip >= chips // 2)
    def _():
        sweep(-1)
        sweep(1)

    totals = totals + line_in[0] + line_in[1]
    roots = jnp.sqrt(totals + 1e-06)
    target = jnp.sum(jnp.where(index < tasks, roots, 0.0), axis=0, keepdims=True) / tasks
    norm = jnp.sum(jnp.where(index == tasks, roots, 0.0), axis=0, keepdims=True)
    rescale = jnp.max(target / norm)

    def scale(source, base, c, chosen=blocks):
        at = row_at(base, c)
        for start, width in chosen:
            span = pl.ds(start, width)
            out[at, span] = source[c, :, span] * rescale

    @pl.loop(0, last)
    def _(c):
        scale(merged, mine_base, c)

    def scale_last():
        scale(merged, mine_base, last)
        if strip:
            out[row_at(other_base, last), high] = strip_merged[...] * rescale

    roles(lambda: scale(merged, mine_base, last, low_blocks), scale_last)

    @pl.loop(0, last)
    def _(c):
        answer(c).wait_recv()
        scale(reply, other_base, c)

    def finish():
        answer(last).wait_recv()
        scale(reply, other_base, last)
        send(last).wait_send()
        answer_low().wait_send()
        if strip:
            answer_strip().wait_recv()
            out[row_at(mine_base, last), high] = strip_reply[...] * rescale
            send_strip().wait_send()

    def finish_other():
        answer_low().wait_recv()
        scale(reply, other_base, last, low_blocks)
        send_low().wait_send()
        answer(last).wait_send()
        if strip:
            answer_strip().wait_send()

    roles(finish, finish_other)

    for s in range(len(steps)):
        exchange(s).wait_send()

    for way in (1, -1):
        @pl.when(has_next[way])
        def _():
            pass_on(way).wait_send()

    for p in range(len(parts)):
        send_head(p).wait_send()

    @pl.loop(0, last)
    def _(c):
        answer(c).wait_send()

        @pl.when(c > 0)
        def _():
            send(c).wait_send()


def shards(mesh, deltas, fishers):
    held, rows, cols = deltas.shape
    assert mesh.shape["task"] == 2 and rows % (2 * ROW_STEP) == 0
    steps = exchange_steps(mesh)
    tasks = held * mesh.shape["task"]
    pieces = rows // 2 // ROW_STEP
    sum_rows = (tasks + 8) // 8 * 8
    f32 = jnp.float32
    dma = pltpu.SemaphoreType.DMA
    strip = cols - strip_cut(cols)
    strip_scratch = [
        pltpu.VMEM((2, ROW_STEP, strip), f32),
        pltpu.VMEM((ROW_STEP, strip), f32),
        pltpu.VMEM((ROW_STEP, strip), f32),
        dma((2,)),
        dma((2,)),
    ] if strip else []
    return pl.pallas_call(
        functools.partial(kernel, steps, mesh.shape["dp"] // CORES, tasks),
        out_shape=pltpu.VMEM((rows, cols), f32),
        in_specs=[pl.BlockSpec(memory_space=pltpu.HBM)] * 2,
        out_specs=pl.BlockSpec(memory_space=pltpu.VMEM),
        scratch_shapes=[
            pltpu.VMEM(deltas.shape, deltas.dtype),
            pltpu.VMEM(fishers.shape, fishers.dtype),
            pltpu.VMEM((pieces, 2, ROW_STEP, cols), f32),
            pltpu.VMEM((pieces, 2, ROW_STEP, cols), f32),
            pltpu.VMEM((pieces, 2, ROW_STEP, cols), f32),
            pltpu.VMEM((pieces, ROW_STEP, cols), f32),
            pltpu.VMEM((pieces, ROW_STEP, cols), f32),
            pltpu.VMEM((held, ROW_STEP, cols), f32),
            pltpu.VMEM((ROW_STEP, cols), f32),
            pltpu.VMEM((len(steps), sum_rows, 128), f32),
            pltpu.VMEM((len(steps), sum_rows, 128), f32),
            dma((2, 2, pieces)),
            dma((pieces,)),
            dma((pieces,)),
            dma((pieces,)),
            dma((pieces,)),
            dma((len(steps),)),
            dma((len(steps),)),
            pltpu.VMEM((2, sum_rows, 128), f32),
            pltpu.VMEM((2, sum_rows, 128), f32),
            dma((2,)),
            dma((2,)),
            dma((2, 2)),
            dma((2,)),
            dma((2,)),
        ] + strip_scratch,
        compiler_params=pltpu.CompilerParams(collective_id=0, has_side_effects=True, vmem_limit_bytes=32 * 1024 * 1024),
        name="merge",
    )(*(pltpu.with_memory_space_constraint(x, pltpu.HBM) for x in (deltas, fishers)))


def solution(mesh):
    placed = (P("task", "dp", "mp"), P("task", "dp", "mp"))
    return jax.shard_map(
        functools.partial(shards, mesh), mesh=mesh, in_specs=placed, out_specs=P("dp", "mp"), check_vma=False
    )
```
